256 devices in a mesh: head: 4 (over z_lo, core), ctx: 64 (over z_hi, x, y).
Axes of the slice: x: 4, y: 4, z: 8 (z_hi: 4, z_lo: 2; z = z_hi * 2 + z_lo), core: 2. Of those that a mesh axis runs over, the one named last changes fastest.
Arguments:
- query: bfloat16 [16384, 16384], P(('head', 'ctx')), may hold values from -5 to 5
- key: bfloat16 [16384, 1024], P(('head', 'ctx')), may hold values from -5 to 5
- value: bfloat16 [16384, 1024], P(('head', 'ctx')), may hold values from -6 to 6
- block_order: int32 [256], replicated, may hold values from 0 to 255, each once
Outputs:
- attended: bfloat16 [16384, 16384], P(('head', 'ctx'))
- log_norm_rows: float32 [16384, 128], P(('head', 'ctx'))
The draws below stay inside these ranges and needn't reach their ends.
All inputs are finite; a program needn't handle non-finite values.
Results may differ from the reference program's by a relative error of at most 0.0036.
Values may be sent and summed in bfloat16 or wider, within the bound.
A program may use at most 64 MiB of HBM per device.

```python
import math
import jax
import jax.numpy as jnp
from jax import lax

HQ = 128
KEY_VALUE_HEADS = 8
HEAD_DIMENSION = 128
BLOCK_ROWS = 64
SEQUENCE_TOKENS = 16384
N_HEAD = 4
N_CTX = 64


def draw_common(key, salt, width):
    fresh = jax.random.fold_in(key, salt)
    base = jnp.clip(jax.random.normal(fresh, (SEQUENCE_TOKENS, width), jnp.float32), -4.5, 4.5)
    return base


def draw_query(key, part):
    return draw_common(key, 3, HQ * HEAD_DIMENSION).astype(jnp.bfloat16)


def draw_key(key, part):
    return draw_common(key, 5, KEY_VALUE_HEADS * HEAD_DIMENSION).astype(jnp.bfloat16)


def shard_levels(own_key, dims, pieces, low, top_value):
    factor_of, own = 1.0, jax.random.fold_in(own_key, 6)
    for position, blocks in pieces:
        heights = jnp.exp(jax.random.uniform(jax.random.fold_in(own, position), (blocks,), jnp.float32, low / len(pieces), top_value / len(pieces)))
        factor_of = factor_of * jnp.repeat(heights, dims[position] // blocks).reshape([-1 if axis == position else 1 for axis in range(len(dims))])
    return factor_of


def noise(key, dims, scale, limit, shards=(), kind=jnp.bfloat16):
    values = jax.random.normal(key, dims, jnp.float32) * scale
    if len(shards) > 0:
        values = shard_levels(key, dims, shards, -0.22, 0.18) * values
    return jnp.clip(values, min=-limit, max=limit).astype(kind)


def setup_inputs(seed: int = 0) -> dict:
    key_list = jax.random.split(jax.random.key(seed), 5)
    return {
        "query": draw_query(jax.random.fold_in(key_list[4], 71), 0),
        "key": draw_key(jax.random.fold_in(key_list[4], 71), 0),
        "value": noise(key_list[2], (SEQUENCE_TOKENS, KEY_VALUE_HEADS * HEAD_DIMENSION), 1.0, 6.0, ((0, 256),)),
        "block_order": jax.random.permutation(key_list[3], SEQUENCE_TOKENS // BLOCK_ROWS).astype(jnp.int32),
    }


def shard_rows(array, shard):
    blocks = array.reshape(N_HEAD, N_CTX, BLOCK_ROWS, array.shape[-1])
    picked = lax.dynamic_index_in_dim(blocks, shard, 1, keepdims=False)
    return picked.reshape(N_HEAD * BLOCK_ROWS, array.shape[-1])

def partial_terms(queries, keys, values, query_positions, key_pos):
    rows = queries.shape[0]
    kv_heads = keys.shape[1] // HEAD_DIMENSION
    group = queries.shape[1] // HEAD_DIMENSION // kv_heads
    scale = 1.0 / math.sqrt(HEAD_DIMENSION)
    qf = queries.astype(jnp.float32).reshape(rows, kv_heads, group, HEAD_DIMENSION)
    kf = keys.astype(jnp.float32).reshape(-1, kv_heads, HEAD_DIMENSION)
    vf = values.astype(jnp.float32).reshape(-1, kv_heads, HEAD_DIMENSION)
    score_matrix = jnp.einsum('rhgd,khd->hgrk', qf, kf, precision=lax.Precision.HIGHEST) * scale
    visible = key_pos[None, :] <= query_positions[:, None]
    shifted = jnp.where(visible, score_matrix, -1e+30)
    peak = jnp.maximum(lax.optimization_barrier(jnp.max(shifted, axis=-1)), -10000.0)
    weights = jnp.exp(shifted - peak[..., None])
    total = lax.optimization_barrier(jnp.sum(weights, axis=-1))
    probs = weights.astype(jnp.bfloat16).astype(jnp.float32)
    acc = jnp.einsum('hgrk,khd->rhgd', probs, vf, precision=lax.Precision.HIGHEST)
    acc = acc.reshape(rows, kv_heads * group * HEAD_DIMENSION)
    peak = peak.transpose(2, 0, 1).reshape(rows, kv_heads * group)
    total = total.transpose(2, 0, 1).reshape(rows, kv_heads * group)
    return (peak, total, acc)

def combine(first, second):
    peak_a, total_a, acc_a = first
    peak_b, total_b, acc_b = second
    peak = jnp.maximum(peak_a, peak_b)
    factor_a = jnp.exp(peak_a - peak)
    factor_b = jnp.exp(peak_b - peak)
    total = total_a * factor_a + total_b * factor_b
    rows, heads = peak.shape
    acc = acc_a.reshape(rows, heads, -1) * factor_a[..., None] + acc_b.reshape(rows, heads, -1) * factor_b[..., None]
    result = (acc / total[..., None]).reshape(rows, -1)
    return (result, peak + jnp.log(total))

def reference(query, key, value, block_order):
    rows = jnp.arange(SEQUENCE_TOKENS, dtype=jnp.int32)
    pos = block_order[rows // BLOCK_ROWS].astype(jnp.int32) * BLOCK_ROWS + rows % BLOCK_ROWS
    pos_col = pos[:, None]

    def one_shard(shard):
        before = (shard - 1) % N_CTX
        queries = shard_rows(query, shard)
        local_positions = shard_rows(pos_col, shard)[:, 0]
        prev_pos = shard_rows(pos_col, before)[:, 0]
        own = partial_terms(queries, shard_rows(key, shard), shard_rows(value, shard), local_positions, local_positions)
        far = partial_terms(queries, shard_rows(key, before), shard_rows(value, before), local_positions, prev_pos)
        result, lse = combine(own, far)
        return (result.astype(jnp.bfloat16), lse)
    results, lses = lax.map(one_shard, jnp.arange(N_CTX, dtype=jnp.int32))
    attended = results.reshape(N_CTX, N_HEAD, BLOCK_ROWS, HQ * HEAD_DIMENSION).transpose(1, 0, 2, 3).reshape(SEQUENCE_TOKENS, HQ * HEAD_DIMENSION)
    log_norm_rows = lses.reshape(N_CTX, N_HEAD, BLOCK_ROWS, HQ).transpose(1, 0, 2, 3).reshape(SEQUENCE_TOKENS, HQ)
    return (attended, log_norm_rows)
```

```python
import functools
import math

import jax
import jax.numpy as jnp
from jax import lax
from jax.experimental import pallas as pl
from jax.experimental.pallas import tpu as pltpu
from jax.sharding import PartitionSpec as P

D = 128
KV = 8
PLANE = 16
SLOTS = 8
HIDDEN = -1e30
MESH = pl.DeviceIdType.MESH


def kernel(n_ctx, order_hbm, q_hbm, k_hbm, v_hbm, out_ref, lse_ref,
           order, q_s, kv, s_s, p_s, o_s, mask_s, l_s, m_s,
           order_sem, q_sem, own_sem, send_sem, recv_sem):
    rows = q_hbm.shape[0]
    width = q_hbm.shape[1] // KV
    group = width // D
    hd = lax.axis_index("head")
    ctx = lax.axis_index("ctx")
    z, c = hd // 2, hd % 2
    nxt, prv = (ctx + 1) % n_ctx, (ctx + n_ctx - 1) % n_ctx
    partner = (2 * z + 1 - c, ctx)
    across = (2 * (1 - z) + c, ctx)
    first = ctx % PLANE == 0
    last = ctx % PLANE == PLANE - 1
    silent = jnp.logical_and(last, z == 0)
    ahead = jnp.logical_not(silent)
    second = jnp.logical_and(last, z == 1)
    own_target = (hd, nxt)
    z_target = (jnp.where(second, c, hd), nxt)
    z_slot = jnp.where(second, 4, 6)
    source = jnp.where(first, 2 + c, hd)

    def chunk(slot, j):
        return kv.at[j, :, pl.ds(slot * rows, rows)]

    def message(kind, j, src, dst, device):
        return pltpu.make_async_remote_copy(
            src_ref=chunk(src, j), dst_ref=chunk(dst, j),
            send_sem=send_sem.at[kind, j], recv_sem=recv_sem.at[dst, j],
            device_id=device, device_id_type=MESH)

    def own_partner(j):
        return message(1, j, 0, 1, partner)

    def own_across(j):
        return message(2, j, 0, 2, across)

    def across_partner(j):
        return message(3, j, 2, 3, partner)

    def own_ahead(j):
        return message(4, j, 0, 4, own_target)

    def far_partner(j):
        return message(5, j, 4, 5, partner)

    def across_ahead(j):
        return message(6, j, 2, z_slot, z_target)

    def far_across(j):
        return message(0, j, 4, 6, across)

    def last_partner(j):
        return message(7, j, 6, 7, partner)

    def arrived(slot, j):
        message(1, j, 0, slot, partner).wait_recv()

    def q_copy(j):
        return pltpu.make_async_copy(
            q_hbm.at[:, pl.ds(pl.multiple_of(j * width, width), width)], q_s.at[j], q_sem.at[j])

    def own_copy(i, j):
        ref = (k_hbm, v_hbm)[i]
        return pltpu.make_async_copy(
            ref.at[:, pl.ds(pl.multiple_of(j * D, D), D)],
            kv.at[j, i, pl.ds(0, rows)], own_sem.at[i, j])

    for j in range(KV):
        own_copy(0, j).start()
        own_copy(1, j).start()
    order_copy = pltpu.make_async_copy(order_hbm, order, order_sem)
    order_copy.start()
    for j in range(KV):
        q_copy(j).start()

    barrier = pltpu.get_barrier_semaphore()

    def greet(device):
        pl.semaphore_signal(barrier, inc=1, device_id=device, device_id_type=MESH)

    greet(partner)
    greet(across)
    greet((source, prv))

    @pl.when(ahead)
    def _():
        greet(own_target)

    @pl.when(second)
    def _():
        greet(z_target)

    peers = 3 + jnp.where(ahead, 1, 0) + jnp.where(second, 1, 0)
    pl.semaphore_wait(barrier, peers)

    for j in range(KV):
        own_copy(0, j).wait()
        own_copy(1, j).wait()
        own_across(j).start()
        if j < 3:
            @pl.when(ahead)
            def _(j=j):
                own_ahead(j).start()
        own_partner(j).start()

    order_copy.wait()
    query_pos = order[hd * n_ctx + ctx] * rows + lax.broadcasted_iota(jnp.int32, (rows, D), 1)
    for slot in range(SLOTS):
        holder = 2 * (z if slot % 4 < 2 else 1 - z) + (c if slot % 2 == 0 else 1 - c)
        block = order[holder * n_ctx + (ctx if slot < 4 else prv)]
        key_pos = block * rows + lax.broadcasted_iota(jnp.int32, (rows, D), 0)
        mask_s[slot * rows:(slot + 1) * rows, :] = jnp.where(
            key_pos <= query_pos, 0.0, HIDDEN).astype(jnp.bfloat16)
    lane = lax.broadcasted_iota(jnp.int32, (rows, D), 1)
    row = lax.broadcasted_iota(jnp.int32, (rows, D), 0)
    pick = jnp.where(lane == row, 1.0, 0.0).astype(jnp.bfloat16)
    picks = jnp.concatenate([pick] * group, axis=0)
    ones = jnp.ones((SLOTS * rows, D), jnp.bfloat16)
    l_s[...] = jnp.ones_like(l_s)
    m_s[...] = jnp.zeros_like(m_s)

    def pass_across(j):
        arrived(2, j)

        @pl.when(ahead)
        def _():
            across_ahead(j).start()

        across_partner(j).start()

    def pass_far(j):
        arrived(4, j)

        @pl.when(first)
        def _():
            far_across(j).start()

        far_partner(j).start()
        arrived(6, j)
        last_partner(j).start()

    pass_across(0)
    pass_across(1)
    pass_far(0)

    scale = 1.0 / math.sqrt(D)
    floor = -10000.0 / scale
    factor = scale * math.log2(math.e)

    def step(j, carry):
        @pl.when(j < KV - 2)
        def _():
            pass_across(j + 2)

        @pl.when(jnp.logical_and(ahead, j < KV - 3))
        def _():
            own_ahead(j + 3).start()

        @pl.when(j < KV - 1)
        def _():
            pass_far(j + 1)

        q_copy(j).wait()
        arrived(1, j)
        arrived(3, j)
        arrived(5, j)
        arrived(7, j)
        heads = [q_s[j, :, i * D:(i + 1) * D] for i in range(group)]
        q = jnp.concatenate([jnp.concatenate(heads, axis=0), picks], axis=1)
        k = jnp.concatenate([kv[j, 0], mask_s[...]], axis=1)
        v = jnp.concatenate([kv[j, 1], ones], axis=1)
        s_s[...] = lax.dot_general(q, k, (((1,), (1,)), ((), ())),
                                   preferred_element_type=jnp.float32)
        total, top = l_s[...], m_s[...]
        peaks = []
        for i in range(group):
            s = s_s[i * rows:(i + 1) * rows, :]
            peak = jnp.maximum(jnp.max(s, axis=1, keepdims=True), floor)
            p_s[i * rows:(i + 1) * rows, :] = jnp.exp2((s - peak) * factor).astype(jnp.bfloat16)
            top = jnp.where(lane == j * group + i, peak, top)
        o_s[...] = jnp.dot(p_s[...], v, preferred_element_type=jnp.float32)
        for i in range(group):
            acc = o_s[i * rows:(i + 1) * rows, :D]
            sums = o_s[i * rows:(i + 1) * rows, D:]
            out_ref[:, pl.ds(pl.multiple_of((j * group + i) * D, D), D)] = (acc / sums).astype(jnp.bfloat16)
            total = jnp.where(lane == j * group + i, sums, total)
        l_s[...] = total
        m_s[...] = top
        return carry

    lax.fori_loop(0, KV, step, 0)
    lse_ref[...] = m_s[...] * scale + jnp.log(l_s[...])

    def drain(j, carry):
        own_across(j).wait_send()
        own_partner(j).wait_send()
        across_partner(j).wait_send()
        far_partner(j).wait_send()
        last_partner(j).wait_send()

        @pl.when(ahead)
        def _():
            own_ahead(j).wait_send()
            across_ahead(j).wait_send()

        @pl.when(first)
        def _():
            far_across(j).wait_send()

        return carry

    lax.fori_loop(0, KV, drain, 0)


def body(query, key, value, block_order):
    n_ctx = lax.axis_size("ctx")
    rows = query.shape[0]
    heads = query.shape[1] // D
    group = heads // KV
    keys = SLOTS * rows
    vmem, smem, hbm = pltpu.VMEM, pltpu.SMEM, pltpu.HBM
    dma = pltpu.SemaphoreType.DMA
    args = [pltpu.with_memory_space_constraint(x, hbm) for x in (block_order, query, key, value)]
    out, lse = pl.pallas_call(
        functools.partial(kernel, n_ctx),
        out_shape=(
            jax.ShapeDtypeStruct(query.shape, jnp.bfloat16),
            jax.ShapeDtypeStruct((rows, heads), jnp.float32),
        ),
        in_specs=[
            pl.BlockSpec(memory_space=hbm),
            pl.BlockSpec(memory_space=hbm),
            pl.BlockSpec(memory_space=hbm),
            pl.BlockSpec(memory_space=hbm),
        ],
        out_specs=(pl.BlockSpec(memory_space=vmem), pl.BlockSpec(memory_space=vmem)),
        scratch_shapes=[
            smem(block_order.shape, jnp.int32),
            vmem((KV, rows, group * D), jnp.bfloat16),
            vmem((KV, 2, keys, D), jnp.bfloat16),
            vmem((group * rows, keys), jnp.float32),
            vmem((group * rows, keys), jnp.bfloat16),
            vmem((group * rows, 2 * D), jnp.float32),
            vmem((keys, D), jnp.bfloat16),
            vmem((rows, heads), jnp.float32),
            vmem((rows, heads), jnp.float32),
            dma,
            dma((KV,)),
            dma((2, KV)),
            dma((8, KV)),
            dma((8, KV)),
        ],
        compiler_params=pltpu.CompilerParams(
            collective_id=0, has_side_effects=True, vmem_limit_bytes=40 * 1024 * 1024
        ),
        cost_estimate=pl.CostEstimate(
            flops=4 * rows * heads * keys * D,
            bytes_accessed=4 * rows * heads * D,
            transcendentals=rows * heads * keys,
        ),
    )(*args)
    return out, lse


def solution(mesh):
    placed = (P(("head", "ctx"), None), P(("head", "ctx"), None), P(("head", "ctx"), None), P())
    return jax.shard_map(
        body,
        mesh=mesh,
        in_specs=placed,
        out_specs=(P(("head", "ctx"), None), P(("head", "ctx"), None)),
        check_vma=False,
    )
```

```python
import functools
import math

import jax
import jax.numpy as jnp
from jax import lax
from jax.experimental import pallas as pl
from jax.experimental.pallas import tpu as pltpu
from jax.sharding import PartitionSpec as P

D = 128
KV = 8
PLANE = 16
AHEAD = 3
LEAD = 2
READY = 4
SLOTS = 8
HIDDEN = -1e30
MESH = pl.DeviceIdType.MESH


def kernel(n_ctx, order_hbm, q_hbm, k_hbm, v_hbm, out_ref, lse_ref,
           order, q_s, kv, s_s, p_s, m_s, o_s, f_s, far_s, mask_s, lse_l, lse_m,
           order_sem, q_sem, own_sem, send_sem, recv_sem):
    rows = q_hbm.shape[0]
    width = q_hbm.shape[1] // KV
    group = width // D
    hd = lax.axis_index("head")
    ctx = lax.axis_index("ctx")
    z, c = hd // 2, hd % 2
    nxt, prv = (ctx + 1) % n_ctx, (ctx + n_ctx - 1) % n_ctx
    partner = (2 * z + 1 - c, ctx)
    across = (2 * (1 - z) + c, ctx)
    first = ctx % PLANE == 0
    last = ctx % PLANE == PLANE - 1
    ahead = jnp.logical_not(jnp.logical_and(last, z == 0))
    second = jnp.logical_and(last, z == 1)
    forwards = jnp.logical_or(first, second)
    crosses = jnp.logical_not(jnp.logical_or(first, last))
    from_cross = jnp.logical_not(jnp.logical_or(first, ctx % PLANE == 1))
    own_target = (hd, nxt)
    cross_target = (2 * (1 - z) + c, nxt)
    z_target = (jnp.where(second, c, hd), nxt)
    z_slot = jnp.where(second, 4, 6)
    source = jnp.where(first, 2 + c, hd)
    cross_source = (2 * (1 - z) + c, prv)

    def chunk(slot, j):
        return kv.at[j, :, pl.ds(slot * rows, rows)]

    def message(kind, j, src, dst, device):
        return pltpu.make_async_remote_copy(
            src_ref=chunk(src, j), dst_ref=chunk(dst, j),
            send_sem=send_sem.at[kind, j], recv_sem=recv_sem.at[dst, j],
            device_id=device, device_id_type=MESH)

    def own_partner(j):
        return message(1, j, 0, 1, partner)

    def own_across(j):
        return message(2, j, 0, 2, across)

    def across_partner(j):
        return message(3, j, 2, 3, partner)

    def own_ahead(j):
        return message(4, j, 0, 4, own_target)

    def far_partner(j):
        return message(5, j, 4, 5, partner)

    def across_ahead(j):
        return message(6, j, 2, z_slot, z_target)

    def own_cross(j):
        return message(6, j, 0, 6, cross_target)

    def far_across(j):
        return message(0, j, 4, 6, across)

    def last_partner(j):
        return message(7, j, 6, 7, partner)

    def arrived(slot, j):
        message(1, j, 0, slot, partner).wait_recv()

    def q_copy(j):
        return pltpu.make_async_copy(
            q_hbm.at[:, pl.ds(pl.multiple_of(j * width, width), width)], q_s.at[j], q_sem.at[j])

    def own_copy(i, j):
        ref = (k_hbm, v_hbm)[i]
        return pltpu.make_async_copy(
            ref.at[:, pl.ds(pl.multiple_of(j * D, D), D)],
            kv.at[j, i, pl.ds(0, rows)], own_sem.at[i, j])

    for j in range(KV):
        own_copy(0, j).start()
        own_copy(1, j).start()
    order_copy = pltpu.make_async_copy(order_hbm, order, order_sem)
    order_copy.start()
    for j in range(KV):
        q_copy(j).start()

    barrier = pltpu.get_barrier_semaphore()

    def greet(device):
        pl.semaphore_signal(barrier, inc=1, device_id=device, device_id_type=MESH)

    greet(partner)
    greet(across)
    greet((source, prv))

    @pl.when(from_cross)
    def _():
        greet(cross_source)

    def one(flag):
        return jnp.where(flag, 1, 0)

    pl.semaphore_wait(barrier, 2 + one(ahead) + one(second) + one(crosses))

    early = jnp.logical_and(ahead, jnp.logical_not(second))
    early = jnp.logical_and(ahead, jnp.logical_not(second))
    for j in range(KV):
        own_copy(0, j).wait()
        own_copy(1, j).wait()
        own_across(j).start()

        @pl.when(crosses)
        def _(j=j):
            own_cross(j).start()

        @pl.when(early if j >= LEAD else ahead)
        def _(j=j):
            own_ahead(j).start()

        own_partner(j).start()

    order_copy.wait()
    query_pos = order[hd * n_ctx + ctx] * rows + lax.broadcasted_iota(jnp.int32, (rows, D), 1)
    for slot in range(SLOTS):
        holder = 2 * (z if slot % 4 < 2 else 1 - z) + (c if slot % 2 == 0 else 1 - c)
        block = order[holder * n_ctx + (ctx if slot < 4 else prv)]
        key_pos = block * rows + lax.broadcasted_iota(jnp.int32, (rows, D), 0)
        mask_s[slot * rows:(slot + 1) * rows, :] = jnp.where(
            key_pos <= query_pos, 0.0, HIDDEN).astype(jnp.bfloat16)
    lane = lax.broadcasted_iota(jnp.int32, (rows, D), 1)
    row = lax.broadcasted_iota(jnp.int32, (rows, D), 0)
    pick = jnp.where(lane == row, 1.0, 0.0).astype(jnp.bfloat16)
    lse_l[...] = jnp.ones_like(lse_l)
    lse_m[...] = jnp.zeros_like(lse_m)

    def pass_across(j):
        arrived(2, j)

        @pl.when(forwards)
        def _():
            across_ahead(j).start()

        @pl.when(jnp.logical_and(second, j < KV - LEAD))
        def _():
            own_ahead(j + LEAD).start()

        across_partner(j).start()

    def pass_far(j):
        arrived(4, j)

        @pl.when(first)
        def _():
            far_across(j).start()

        far_partner(j).start()

    def pass_last(j):
        arrived(6, j)
        last_partner(j).start()

    scale = 1.0 / math.sqrt(D)
    floor = -10000.0 / scale
    factor = scale * math.log2(math.e)
    keys = SLOTS // 2 * rows
    parts = [range(group // 2), range(group // 2, group)]
    picks = jnp.concatenate([pick] * (group // 2), axis=0)
    ones = jnp.ones((keys, D), jnp.bfloat16)

    def scores(j, shard):
        seen = pl.ds(shard * keys, keys)
        k = jnp.concatenate([kv[j, 0, seen], mask_s[seen]], axis=1)
        for part, heads in enumerate(parts):
            q = jnp.concatenate([q_s[j, :, i * D:(i + 1) * D] for i in heads], axis=0)
            s_s[part] = lax.dot_general(
                jnp.concatenate([q, picks], axis=1), k, (((1,), (1,)), ((), ())),
                preferred_element_type=jnp.float32)

    def value(j, shard):
        return jnp.concatenate([kv[j, 1, shard * keys:(shard + 1) * keys], ones], axis=1)

    def own_step(j, carry):
        @pl.when(j < KV - 2)
        def _():
            pass_across(j + 2)

        @pl.when(jnp.logical_and(jnp.logical_not(first), j >= KV - READY))
        def _():
            pass_far(j - (KV - READY))
            pass_last(j - (KV - READY))

        q_copy(j).wait()
        arrived(1, j)
        arrived(3, j)
        scores(j, 0)
        v = value(j, 0)
        for part, heads in enumerate(parts):
            for n, i in enumerate(heads):
                at = slice(n * rows, (n + 1) * rows)
                s = s_s[part, at]
                peak = jnp.maximum(jnp.max(s, axis=1, keepdims=True), floor)
                p_s[part, at] = jnp.exp2((s - peak) * factor).astype(jnp.bfloat16)
                m_s[j, i] = jnp.broadcast_to(peak, (rows, D))
            o_s[j, part] = jnp.dot(p_s[part], v, preferred_element_type=jnp.float32)
        return carry

    def far_step(j, carry):
        later = jnp.logical_not(first)

        @pl.when(jnp.logical_and(first, j < KV - AHEAD))
        def _():
            pass_far(j + AHEAD)

        @pl.when(jnp.logical_and(later, jnp.logical_and(j >= READY - 1, j < KV - 1)))
        def _():
            pass_far(j + 1)

        @pl.when(jnp.logical_and(jnp.logical_or(first, j >= READY - 1), j < KV - 1))
        def _():
            pass_last(j + 1)

        arrived(5, j)
        arrived(7, j)
        scores(j, 1)
        v = value(j, 1)
        total, top = lse_l[...], lse_m[...]
        for part, heads in enumerate(parts):
            for n, i in enumerate(heads):
                at = slice(n * rows, (n + 1) * rows)
                s = s_s[part, at]
                peak = jnp.maximum(m_s[j, i], jnp.max(s, axis=1, keepdims=True))
                p = [jnp.exp2((s[:, at * D:(at + 1) * D] - peak) * factor).astype(jnp.bfloat16)
                     for at in range(keys // D)]
                p_s[part, at] = jnp.concatenate(p, axis=1)
                f_s[part, at] = jnp.exp2((m_s[j, i] - peak) * factor)
                top = jnp.where(lane == j * group + i, peak, top)
            far_s[part] = jnp.dot(p_s[part], v, preferred_element_type=jnp.float32)
        for part, heads in enumerate(parts):
            for n, i in enumerate(heads):
                at = slice(n * rows, (n + 1) * rows)
                kept = f_s[part, at]
                acc = o_s[j, part, at, :D] * kept + far_s[part, at, :D]
                sums = o_s[j, part, at, D:] * kept + far_s[part, at, D:]
                out_ref[:, pl.ds(pl.multiple_of((j * group + i) * D, D), D)] = (
                    acc / sums).astype(jnp.bfloat16)
                total = jnp.where(lane == j * group + i, sums, total)
        lse_l[...] = total
        lse_m[...] = top
        return carry

    pass_across(0)
    pass_across(1)
    lax.fori_loop(0, KV, own_step, 0)

    @pl.when(first)
    def _():
        for j in range(AHEAD):
            pass_far(j)
        pass_last(0)

    lax.fori_loop(0, KV, far_step, 0)
    lse_ref[...] = lse_m[...] * scale + jnp.log(lse_l[...])

    def drain(j, carry):
        own_across(j).wait_send()
        own_partner(j).wait_send()
        across_partner(j).wait_send()
        far_partner(j).wait_send()
        last_partner(j).wait_send()

        @pl.when(ahead)
        def _():
            own_ahead(j).wait_send()

        @pl.when(crosses)
        def _():
            own_cross(j).wait_send()

        @pl.when(forwards)
        def _():
            across_ahead(j).wait_send()

        @pl.when(first)
        def _():
            far_across(j).wait_send()

        return carry

    lax.fori_loop(0, KV, drain, 0)


def body(query, key, value, block_order):
    n_ctx = lax.axis_size("ctx")
    rows = query.shape[0]
    heads = query.shape[1] // D
    group = heads // KV
    keys = SLOTS * rows
    half = group * rows // 2
    vmem, smem, hbm = pltpu.VMEM, pltpu.SMEM, pltpu.HBM
    dma = pltpu.SemaphoreType.DMA
    args = [pltpu.with_memory_space_constraint(x, hbm) for x in (block_order, query, key, value)]
    out, lse = pl.pallas_call(
        functools.partial(kernel, n_ctx),
        out_shape=(
            jax.ShapeDtypeStruct(query.shape, jnp.bfloat16),
            jax.ShapeDtypeStruct((rows, heads), jnp.float32),
        ),
        in_specs=[
            pl.BlockSpec(memory_space=hbm),
            pl.BlockSpec(memory_space=hbm),
            pl.BlockSpec(memory_space=hbm),
            pl.BlockSpec(memory_space=hbm),
        ],
        out_specs=(pl.BlockSpec(memory_space=vmem), pl.BlockSpec(memory_space=vmem)),
        scratch_shapes=[
            smem(block_order.shape, jnp.int32),
            vmem((KV, rows, group * D), jnp.bfloat16),
            vmem((KV, 2, keys, D), jnp.bfloat16),
            vmem((2, half, keys // 2), jnp.float32),
            vmem((2, half, keys // 2), jnp.bfloat16),
            vmem((KV, group, rows, D), jnp.float32),
            vmem((KV, 2, half, 2 * D), jnp.float32),
            vmem((2, half, D), jnp.float32),
            vmem((2, half, 2 * D), jnp.float32),
            vmem((keys, D), jnp.bfloat16),
            vmem((rows, heads), jnp.float32),
            vmem((rows, heads), jnp.float32),
            dma,
            dma((KV,)),
            dma((2, KV)),
            dma((8, KV)),
            dma((8, KV)),
        ],
        compiler_params=pltpu.CompilerParams(
            collective_id=0, has_side_effects=True, vmem_limit_bytes=40 * 1024 * 1024
        ),
        cost_estimate=pl.CostEstimate(
            flops=4 * rows * heads * keys * D,
            bytes_accessed=4 * rows * heads * D,
            transcendentals=rows * heads * keys,
        ),
    )(*args)
    return out, lse


def solution(mesh):
    placed = (P(("head", "ctx"), None), P(("head", "ctx"), None), P(("head", "ctx"), None), P())
    return jax.shard_map(
        body,
        mesh=mesh,
        in_specs=placed,
        out_specs=(P(("head", "ctx"), None), P(("head", "ctx"), None)),
        check_vma=False,
    )
```

```python
import functools
import math

import jax
import jax.numpy as jnp
from jax import lax
from jax.experimental import pallas as pl
from jax.experimental.pallas import tpu as pltpu
from jax.sharding import PartitionSpec as P

D = 128
KV = 8
PLANE = 16
AHEAD = 3
RELAY = 3
READY = 4
SLOTS = 8
HIDDEN = -1e30
MESH = pl.DeviceIdType.MESH


def kernel(n_ctx, order_hbm, q_hbm, k_hbm, v_hbm, out_ref, lse_l, lse_m,
           order, q_s, kv, relay_s, s_s, p_s, m_s, o_s, f_s, far_s, mask_s,
           order_sem, q_sem, own_sem, send_sem, recv_sem):
    rows = q_hbm.shape[0]
    width = q_hbm.shape[1] // KV
    group = width // D
    hd = lax.axis_index("head")
    ctx = lax.axis_index("ctx")
    z, c = hd // 2, hd % 2
    nxt, prv = (ctx + 1) % n_ctx, (ctx + n_ctx - 1) % n_ctx
    partner = (2 * z + 1 - c, ctx)
    across = (2 * (1 - z) + c, ctx)
    first = ctx % PLANE == 0
    last = ctx % PLANE == PLANE - 1
    ahead = jnp.logical_not(jnp.logical_and(last, z == 0))
    second = jnp.logical_and(last, z == 1)
    spare = ctx % PLANE == RELAY
    relays = jnp.logical_and(spare, z == 1)
    by_relay = jnp.logical_and(first, z == 1)
    forwards = jnp.logical_or(jnp.logical_or(first, spare), second)
    crosses = jnp.logical_not(jnp.logical_or(jnp.logical_or(first, spare), last))
    from_cross = jnp.logical_not(jnp.logical_or(
        first, jnp.logical_or(ctx % PLANE == 1, ctx % PLANE == RELAY + 1)))
    own_target = (hd, nxt)
    cross_target = (2 * (1 - z) + c, nxt)
    z_target = (jnp.where(second, c, hd), nxt)
    z_slot = jnp.where(second, 4, 6)
    source = (jnp.where(first, 2 + c, hd), jnp.where(by_relay, prv - (PLANE - 1 - RELAY), prv))
    relay_source = (hd, ctx + PLANE - 1 - RELAY)
    relay_stop = (hd, ctx - (PLANE - 1 - RELAY))
    relay_target = (hd, (ctx + PLANE - RELAY) % n_ctx)
    cross_source = (2 * (1 - z) + c, prv)

    def chunk(slot, j):
        return kv.at[j, :, pl.ds(slot * rows, rows)]

    def message(kind, j, src, dst, device):
        return pltpu.make_async_remote_copy(
            src_ref=chunk(src, j), dst_ref=chunk(dst, j),
            send_sem=send_sem.at[kind, j], recv_sem=recv_sem.at[dst, j],
            device_id=device, device_id_type=MESH)

    def own_partner(j):
        return message(1, j, 0, 1, partner)

    def own_across(j):
        return message(2, j, 0, 2, across)

    def across_partner(j):
        return message(3, j, 2, 3, partner)

    def own_ahead(j):
        return message(4, j, 0, 4, own_target)

    def far_partner(j):
        return message(5, j, 4, 5, partner)

    def across_ahead(j):
        return message(6, j, 2, z_slot, z_target)

    def to_relay(j):
        return pltpu.make_async_remote_copy(
            src_ref=chunk(0, j), dst_ref=relay_s.at[j],
            send_sem=send_sem.at[4, j], recv_sem=recv_sem.at[8, j],
            device_id=relay_stop, device_id_type=MESH)

    def from_relay(j):
        return pltpu.make_async_remote_copy(
            src_ref=relay_s.at[j], dst_ref=chunk(4, j),
            send_sem=send_sem.at[8, j], recv_sem=recv_sem.at[4, j],
            device_id=relay_target, device_id_type=MESH)

    def own_cross(j):
        return message(6, j, 0, 6, cross_target)

    def far_across(j):
        return message(0, j, 4, 6, across)

    def last_partner(j):
        return message(7, j, 6, 7, partner)

    def arrived(slot, j):
        message(1, j, 0, slot, partner).wait_recv()

    def q_copy(j):
        return pltpu.make_async_copy(
            q_hbm.at[:, pl.ds(pl.multiple_of(j * width, width), width)], q_s.at[j], q_sem.at[j])

    def own_copy(i, j):
        ref = (k_hbm, v_hbm)[i]
        return pltpu.make_async_copy(
            ref.at[:, pl.ds(pl.multiple_of(j * D, D), D)],
            kv.at[j, i, pl.ds(0, rows)], own_sem.at[i, j])

    for j in range(KV):
        own_copy(0, j).start()
        own_copy(1, j).start()
    order_copy = pltpu.make_async_copy(order_hbm, order, order_sem)
    order_copy.start()
    for j in range(KV):
        q_copy(j).start()

    barrier = pltpu.get_barrier_semaphore()

    def greet(device):
        pl.semaphore_signal(barrier, inc=1, device_id=device, device_id_type=MESH)

    greet(partner)
    greet(across)
    greet(source)

    @pl.when(relays)
    def _():
        greet(relay_source)

    @pl.when(from_cross)
    def _():
        greet(cross_source)

    def one(flag):
        return jnp.where(flag, 1, 0)

    pl.semaphore_wait(barrier, 2 + one(ahead) + one(second) + one(crosses) + one(relays))

    early = jnp.logical_and(ahead, jnp.logical_not(second))
    early = jnp.logical_and(ahead, jnp.logical_not(second))
    for j in range(KV):
        own_copy(0, j).wait()
        own_copy(1, j).wait()
        own_across(j).start()

        @pl.when(crosses)
        def _(j=j):
            own_cross(j).start()

        @pl.when(early)
        def _(j=j):
            own_ahead(j).start()

        @pl.when(second)
        def _(j=j):
            to_relay(j).start()

        own_partner(j).start()

    order_copy.wait()
    query_pos = order[hd * n_ctx + ctx] * rows + lax.broadcasted_iota(jnp.int32, (rows, D), 1)
    for slot in range(SLOTS):
        holder = 2 * (z if slot % 4 < 2 else 1 - z) + (c if slot % 2 == 0 else 1 - c)
        block = order[holder * n_ctx + (ctx if slot < 4 else prv)]
        key_pos = block * rows + lax.broadcasted_iota(jnp.int32, (rows, D), 0)
        mask_s[slot * rows:(slot + 1) * rows, :] = jnp.where(
            key_pos <= query_pos, 0.0, HIDDEN).astype(jnp.bfloat16)
    lane = lax.broadcasted_iota(jnp.int32, (rows, D), 1)
    row = lax.broadcasted_iota(jnp.int32, (rows, D), 0)
    pick = jnp.where(lane == row, 1.0, 0.0).astype(jnp.bfloat16)
    lse_l[...] = jnp.ones_like(lse_l)
    lse_m[...] = jnp.zeros_like(lse_m)

    def pass_across(j):
        arrived(2, j)

        @pl.when(forwards)
        def _():
            across_ahead(j).start()

        across_partner(j).start()

    def pass_far(j):
        arrived(4, j)

        @pl.when(first)
        def _():
            far_across(j).start()

        far_partner(j).start()

    def pass_relay(j):
        to_relay(j).wait_recv()
        from_relay(j).start()

    def pass_last(j):
        arrived(6, j)
        last_partner(j).start()

    scale = 1.0 / math.sqrt(D)
    floor = -10000.0 / scale
    factor = scale * math.log2(math.e)
    keys = SLOTS // 2 * rows
    parts = [range(group // 2), range(group // 2, group)]
    picks = jnp.concatenate([pick] * (group // 2), axis=0)
    ones = jnp.ones((keys, D), jnp.bfloat16)

    def scores(j, shard):
        seen = pl.ds(shard * keys, keys)
        k = jnp.concatenate([kv[j, 0, seen], mask_s[seen]], axis=1)
        for part, heads in enumerate(parts):
            q = jnp.concatenate([q_s[j, :, i * D:(i + 1) * D] for i in heads], axis=0)
            s_s[part] = lax.dot_general(
                jnp.concatenate([q, picks], axis=1), k, (((1,), (1,)), ((), ())),
                preferred_element_type=jnp.float32)

    def value(j, shard):
        return jnp.concatenate([kv[j, 1, shard * keys:(shard + 1) * keys], ones], axis=1)

    def own_step(j, carry):
        @pl.when(j < KV - 2)
        def _():
            pass_across(j + 2)

            @pl.when(relays)
            def _():
                pass_relay(j + 2)

        @pl.when(jnp.logical_and(jnp.logical_not(first), j >= KV - READY))
        def _():
            pass_far(j - (KV - READY))
            pass_last(j - (KV - READY))

        q_copy(j).wait()
        arrived(1, j)
        arrived(3, j)
        scores(j, 0)
        v = value(j, 0)
        for part, heads in enumerate(parts):
            for n, i in enumerate(heads):
                at = slice(n * rows, (n + 1) * rows)
                s = s_s[part, at]
                peak = jnp.maximum(jnp.max(s, axis=1, keepdims=True), floor)
                p_s[part, at] = jnp.exp2((s - peak) * factor).astype(jnp.bfloat16)
                m_s[j, i] = jnp.broadcast_to(peak, (rows, D))
            o_s[j, part] = jnp.dot(p_s[part], v, preferred_element_type=jnp.float32)
        return carry

    def far_step(j, carry):
        later = jnp.logical_not(first)

        @pl.when(jnp.logical_and(first, j < KV - AHEAD))
        def _():
            pass_far(j + AHEAD)

        @pl.when(jnp.logical_and(later, jnp.logical_and(j >= READY - 1, j < KV - 1)))
        def _():
            pass_far(j + 1)

        @pl.when(jnp.logical_and(jnp.logical_or(first, j >= READY - 1), j < KV - 1))
        def _():
            pass_last(j + 1)

        arrived(5, j)
        arrived(7, j)
        scores(j, 1)
        v = value(j, 1)
        total, top = lse_l[...], lse_m[...]
        for part, heads in enumerate(parts):
            for n, i in enumerate(heads):
                at = slice(n * rows, (n + 1) * rows)
                s = s_s[part, at]
                peak = jnp.maximum(m_s[j, i], jnp.max(s, axis=1, keepdims=True))
                p = [jnp.exp2((s[:, at * D:(at + 1) * D] - peak) * factor).astype(jnp.bfloat16)
                     for at in range(keys // D)]
                p_s[part, at] = jnp.concatenate(p, axis=1)
                f_s[part, at] = jnp.exp2((m_s[j, i] - peak) * factor)
                top = jnp.where(lane == j * group + i, peak, top)
            far_s[part] = jnp.dot(p_s[part], v, preferred_element_type=jnp.float32)
        for part, heads in enumerate(parts):
            for n, i in enumerate(heads):
                at = slice(n * rows, (n + 1) * rows)
                kept = f_s[part, at]
                acc = o_s[j, part, at, :D] * kept + far_s[part, at, :D]
                sums = o_s[j, part, at, D:] * kept + far_s[part, at, D:]
                out_ref[:, pl.ds(pl.multiple_of((j * group + i) * D, D), D)] = (
                    acc / sums).astype(jnp.bfloat16)
                total = jnp.where(lane == j * group + i, sums, total)
        lse_l[...] = total
        lse_m[...] = top
        return carry

    for j in range(2):
        pass_across(j)

        @pl.when(relays)
        def _(j=j):
            pass_relay(j)

    lax.fori_loop(0, KV, own_step, 0)

    @pl.when(first)
    def _():
        for j in range(AHEAD):
            pass_far(j)
        pass_last(0)

    lax.fori_loop(0, KV, far_step, 0)
    def drain(j, carry):
        own_across(j).wait_send()
        own_partner(j).wait_send()
        across_partner(j).wait_send()
        far_partner(j).wait_send()
        last_partner(j).wait_send()

        @pl.when(ahead)
        def _():
            own_ahead(j).wait_send()

        @pl.when(relays)
        def _():
            from_relay(j).wait_send()

        @pl.when(crosses)
        def _():
            own_cross(j).wait_send()

        @pl.when(forwards)
        def _():
            across_ahead(j).wait_send()

        @pl.when(first)
        def _():
            far_across(j).wait_send()

        return carry

    lax.fori_loop(0, KV, drain, 0)


def finish(out_ref, total, top, out_hbm, lse_hbm, lse_s, out_sem, lse_sem):
    width = out_ref.shape[1] // KV
    copies = [
        pltpu.make_async_copy(
            out_ref.at[:, j * width:(j + 1) * width],
            out_hbm.at[:, j * width:(j + 1) * width], out_sem.at[j])
        for j in range(KV)
    ]
    for copy in copies:
        copy.start()
    lse_s[...] = top[...] * (1.0 / math.sqrt(D)) + jnp.log(total[...])
    lse_copy = pltpu.make_async_copy(lse_s, lse_hbm, lse_sem)
    lse_copy.start()
    for copy in copies:
        copy.wait()
    lse_copy.wait()


def body(query, key, value, block_order):
    n_ctx = lax.axis_size("ctx")
    rows = query.shape[0]
    heads = query.shape[1] // D
    group = heads // KV
    keys = SLOTS * rows
    half = group * rows // 2
    vmem, smem, hbm = pltpu.VMEM, pltpu.SMEM, pltpu.HBM
    dma = pltpu.SemaphoreType.DMA
    args = [pltpu.with_memory_space_constraint(x, hbm) for x in (block_order, query, key, value)]
    stats = jax.ShapeDtypeStruct((rows, heads), jnp.float32)
    out, total, top = pl.pallas_call(
        functools.partial(kernel, n_ctx),
        out_shape=(
            jax.ShapeDtypeStruct(query.shape, jnp.bfloat16),
            stats,
            stats,
        ),
        in_specs=[
            pl.BlockSpec(memory_space=hbm),
            pl.BlockSpec(memory_space=hbm),
            pl.BlockSpec(memory_space=hbm),
            pl.BlockSpec(memory_space=hbm),
        ],
        out_specs=(pl.BlockSpec(memory_space=vmem),) * 3,
        scratch_shapes=[
            smem(block_order.shape, jnp.int32),
            vmem((KV, rows, group * D), jnp.bfloat16),
            vmem((KV, 2, keys, D), jnp.bfloat16),
            vmem((KV, 2, rows, D), jnp.bfloat16),
            vmem((2, half, keys // 2), jnp.float32),
            vmem((2, half, keys // 2), jnp.bfloat16),
            vmem((KV, group, rows, D), jnp.float32),
            vmem((KV, 2, half, 2 * D), jnp.float32),
            vmem((2, half, D), jnp.float32),
            vmem((2, half, 2 * D), jnp.float32),
            vmem((keys, D), jnp.bfloat16),
            dma,
            dma((KV,)),
            dma((2, KV)),
            dma((9, KV)),
            dma((9, KV)),
        ],
        compiler_params=pltpu.CompilerParams(
            collective_id=0, has_side_effects=True, vmem_limit_bytes=40 * 1024 * 1024
        ),
        cost_estimate=pl.CostEstimate(
            flops=4 * rows * heads * keys * D,
            bytes_accessed=4 * rows * heads * D,
            transcendentals=rows * heads * keys,
        ),
    )(*args)
    return pl.pallas_call(
        finish,
        out_shape=(jax.ShapeDtypeStruct(query.shape, jnp.bfloat16), stats),
        in_specs=[pl.BlockSpec(memory_space=vmem)] * 3,
        out_specs=(pl.BlockSpec(memory_space=hbm),) * 2,
        scratch_shapes=[vmem((rows, heads), jnp.float32), dma((KV,)), dma],
        compiler_params=pltpu.CompilerParams(vmem_limit_bytes=4 * 1024 * 1024),
    )(out, total, top)


def solution(mesh):
    placed = (P(("head", "ctx"), None), P(("head", "ctx"), None), P(("head", "ctx"), None), P())
    return jax.shard_map(
        body,
        mesh=mesh,
        in_specs=placed,
        out_specs=(P(("head", "ctx"), None), P(("head", "ctx"), None)),
        check_vma=False,
    )
```

```python
import functools
import math

import jax
import jax.numpy as jnp
from jax import lax
from jax.experimental import pallas as pl
from jax.experimental.pallas import tpu as pltpu
from jax.sharding import PartitionSpec as P

D = 128
KV = 8
PLANE = 16
AHEAD = 5
RELAY = 3
DIRECT = 6
READY = 4
SLOTS = 8
HIDDEN = -1e30
MESH = pl.DeviceIdType.MESH


def kernel(n_ctx, order_hbm, q_hbm, k_hbm, v_hbm, out_ref, lse_l, lse_m,
           order, q_s, kv, relay_s, s_s, p_s, m_s, o_s, f_s, far_s, mask_s,
           order_sem, q_sem, own_sem, send_sem, recv_sem):
    rows = q_hbm.shape[0]
    width = q_hbm.shape[1] // KV
    group = width // D
    hd = lax.axis_index("head")
    ctx = lax.axis_index("ctx")
    z, c = hd // 2, hd % 2
    nxt, prv = (ctx + 1) % n_ctx, (ctx + n_ctx - 1) % n_ctx
    partner = (2 * z + 1 - c, ctx)
    across = (2 * (1 - z) + c, ctx)
    diagonal = (2 * (1 - z) + 1 - c, ctx)
    first = ctx % PLANE == 0
    last = ctx % PLANE == PLANE - 1
    shard = ctx % PLANE
    spare = shard == RELAY
    relays = jnp.logical_and(spare, z == 1)
    split = jnp.logical_and(last, z == 1)
    ahead = jnp.logical_not(split)
    crowded = jnp.logical_and(last, z == 0)
    by_relay = jnp.logical_and(first, z == 1)
    forwards = jnp.logical_or(first, spare)
    crosses = jnp.logical_not(jnp.logical_or(forwards, last))
    before = prv % PLANE
    from_cross = jnp.logical_not(jnp.logical_or(
        jnp.logical_or(before == 0, before == PLANE - 1), before == RELAY))
    own_target = (hd, nxt)
    cross_target = (2 * (1 - z) + c, nxt)
    cross_source = (2 * (1 - z) + c, prv)
    source = (hd, jnp.where(by_relay, prv - (PLANE - 1 - RELAY), prv))
    relay_source = (hd, ctx - shard + PLANE - 1)
    relay_target = (hd, (ctx - shard + PLANE) % n_ctx)

    def chunk(slot, j):
        return kv.at[j, :, pl.ds(slot * rows, rows)]

    def message(kind, j, src, dst, device):
        return pltpu.make_async_remote_copy(
            src_ref=chunk(src, j), dst_ref=chunk(dst, j),
            send_sem=send_sem.at[kind, j], recv_sem=recv_sem.at[dst, j],
            device_id=device, device_id_type=MESH)

    def own_partner(j):
        return message(1, j, 0, 1, partner)

    def own_across(j):
        return message(2, j, 0, 2, across)

    def across_partner(j):
        return message(3, j, 2, 3, partner)

    def own_ahead(j):
        return message(4, j, 0, 4, own_target)

    def far_partner(j):
        return message(5, j, 4, 5, partner)

    def across_ahead(j):
        return message(6, j, 2, 6, own_target)

    def to_relay(j):
        stop = ctx - (PLANE - 1 - RELAY)
        return pltpu.make_async_remote_copy(
            src_ref=chunk(0, j), dst_ref=relay_s.at[j],
            send_sem=send_sem.at[4, j], recv_sem=recv_sem.at[8, j],
            device_id=(hd, stop), device_id_type=MESH)

    def from_relay(j):
        return pltpu.make_async_remote_copy(
            src_ref=relay_s.at[j], dst_ref=chunk(4, j),
            send_sem=send_sem.at[8, j], recv_sem=recv_sem.at[4, j],
            device_id=relay_target, device_id_type=MESH)

    def own_cross(j):
        return message(6, j, 0, 6, cross_target)

    def far_across(j):
        return message(0, j, 4, 6, across)

    def last_partner(j):
        return message(7, j, 6, 7, partner)

    def far_diagonal(j):
        return message(7, j, 4, 7, diagonal)

    def direct(j):
        return jnp.logical_and(first, j >= DIRECT)

    def arrived(slot, j):
        message(1, j, 0, slot, partner).wait_recv()

    def q_copy(j):
        return pltpu.make_async_copy(
            q_hbm.at[:, pl.ds(pl.multiple_of(j * width, width), width)], q_s.at[j], q_sem.at[j])

    def own_copy(i, j):
        ref = (k_hbm, v_hbm)[i]
        return pltpu.make_async_copy(
            ref.at[:, pl.ds(pl.multiple_of(j * D, D), D)],
            kv.at[j, i, pl.ds(0, rows)], own_sem.at[i, j])

    for j in range(KV):
        own_copy(0, j).start()
        own_copy(1, j).start()
    order_copy = pltpu.make_async_copy(order_hbm, order, order_sem)
    order_copy.start()
    for j in range(KV):
        q_copy(j).start()

    barrier = pltpu.get_barrier_semaphore()

    def greet(device):
        pl.semaphore_signal(barrier, inc=1, device_id=device, device_id_type=MESH)

    greet(partner)
    greet(across)
    greet(source)

    @pl.when(relays)
    def _():
        greet(relay_source)

    @pl.when(first)
    def _():
        greet(diagonal)

    @pl.when(from_cross)
    def _():
        greet(cross_source)

    def one(flag):
        return jnp.where(flag, 1, 0)

    pl.semaphore_wait(
        barrier, 2 + one(ahead) + one(split) + one(crosses) + one(relays) + one(first))

    for j in range(KV):
        own_copy(0, j).wait()
        own_copy(1, j).wait()

        @pl.when(jnp.logical_not(crowded))
        def _(j=j):
            own_across(j).start()

        @pl.when(crosses)
        def _(j=j):
            own_cross(j).start()

        @pl.when(ahead)
        def _(j=j):
            own_ahead(j).start()

        @pl.when(split)
        def _(j=j):
            to_relay(j).start()

        own_partner(j).start()

    @pl.when(crowded)
    def _():
        for j in range(KV):
            own_across(j).start()

    order_copy.wait()
    query_pos = order[hd * n_ctx + ctx] * rows + lax.broadcasted_iota(jnp.int32, (rows, D), 1)
    for slot in range(SLOTS):
        holder = 2 * (z if slot % 4 < 2 else 1 - z) + (c if slot % 2 == 0 else 1 - c)
        block = order[holder * n_ctx + (ctx if slot < 4 else prv)]
        key_pos = block * rows + lax.broadcasted_iota(jnp.int32, (rows, D), 0)
        mask_s[slot * rows:(slot + 1) * rows, :] = jnp.where(
            key_pos <= query_pos, 0.0, HIDDEN).astype(jnp.bfloat16)
    lane = lax.broadcasted_iota(jnp.int32, (rows, D), 1)
    row = lax.broadcasted_iota(jnp.int32, (rows, D), 0)
    pick = jnp.where(lane == row, 1.0, 0.0).astype(jnp.bfloat16)
    lse_l[...] = jnp.ones_like(lse_l)
    lse_m[...] = jnp.zeros_like(lse_m)

    def pass_across(j):
        arrived(2, j)

        @pl.when(forwards)
        def _():
            across_ahead(j).start()

        across_partner(j).start()

    def pass_far(j):
        arrived(4, j)

        @pl.when(first)
        def _():
            far_across(j).start()

        @pl.when(direct(j))
        def _():
            far_diagonal(j).start()

        far_partner(j).start()

    def pass_relay(j):
        to_relay(j).wait_recv()
        from_relay(j).start()

    def pass_last(j):
        @pl.when(jnp.logical_not(direct(j)))
        def _():
            arrived(6, j)
            last_partner(j).start()

    scale = 1.0 / math.sqrt(D)
    floor = -10000.0 / scale
    factor = scale * math.log2(math.e)
    keys = SLOTS // 2 * rows
    parts = [range(group // 2), range(group // 2, group)]
    picks = jnp.concatenate([pick] * (group // 2), axis=0)
    ones = jnp.ones((keys, D), jnp.bfloat16)

    def scores(j, shard):
        seen = pl.ds(shard * keys, keys)
        k = jnp.concatenate([kv[j, 0, seen], mask_s[seen]], axis=1)
        for part, heads in enumerate(parts):
            q = jnp.concatenate([q_s[j, :, i * D:(i + 1) * D] for i in heads], axis=0)
            s_s[part] = lax.dot_general(
                jnp.concatenate([q, picks], axis=1), k, (((1,), (1,)), ((), ())),
                preferred_element_type=jnp.float32)

    def value(j, shard):
        return jnp.concatenate([kv[j, 1, shard * keys:(shard + 1) * keys], ones], axis=1)

    def own_step(j, carry):
        @pl.when(j < KV - 2)
        def _():
            pass_across(j + 2)

            @pl.when(relays)
            def _():
                pass_relay(j + 2)

        @pl.when(jnp.logical_and(jnp.logical_not(first), j >= KV - READY))
        def _():
            pass_far(j - (KV - READY))
            pass_last(j - (KV - READY))

        q_copy(j).wait()
        arrived(1, j)
        arrived(3, j)
        scores(j, 0)
        v = value(j, 0)
        for part, heads in enumerate(parts):
            for n, i in enumerate(heads):
                at = slice(n * rows, (n + 1) * rows)
                s = s_s[part, at]
                peak = jnp.maximum(jnp.max(s, axis=1, keepdims=True), floor)
                p_s[part, at] = jnp.exp2((s - peak) * factor).astype(jnp.bfloat16)
                m_s[j, i] = jnp.broadcast_to(peak, (rows, D))
            o_s[j, part] = jnp.dot(p_s[part], v, preferred_element_type=jnp.float32)
        return carry

    def far_step(j, carry):
        later = jnp.logical_not(first)

        @pl.when(jnp.logical_and(first, j < KV - AHEAD))
        def _():
            pass_far(j + AHEAD)

        @pl.when(jnp.logical_and(later, jnp.logical_and(j >= READY - 1, j < KV - 1)))
        def _():
            pass_far(j + 1)

        @pl.when(jnp.logical_and(jnp.logical_or(first, j >= READY - 1), j < KV - 1))
        def _():
            pass_last(j + 1)

        @pl.when(direct(j))
        def _():
            arrived(6, j)

        arrived(5, j)
        arrived(7, j)
        scores(j, 1)
        v = value(j, 1)
        total, top = lse_l[...], lse_m[...]
        for part, heads in enumerate(parts):
            for n, i in enumerate(heads):
                at = slice(n * rows, (n + 1) * rows)
                s = s_s[part, at]
                peak = jnp.maximum(m_s[j, i], jnp.max(s, axis=1, keepdims=True))
                p = [jnp.exp2((s[:, at * D:(at + 1) * D] - peak) * factor).astype(jnp.bfloat16)
                     for at in range(keys // D)]
                p_s[part, at] = jnp.concatenate(p, axis=1)
                f_s[part, at] = jnp.exp2((m_s[j, i] - peak) * factor)
                top = jnp.where(lane == j * group + i, peak, top)
            far_s[part] = jnp.dot(p_s[part], v, preferred_element_type=jnp.float32)
        for part, heads in enumerate(parts):
            for n, i in enumerate(heads):
                at = slice(n * rows, (n + 1) * rows)
                kept = f_s[part, at]
                acc = o_s[j, part, at, :D] * kept + far_s[part, at, :D]
                sums = o_s[j, part, at, D:] * kept + far_s[part, at, D:]
                out_ref[:, pl.ds(pl.multiple_of((j * group + i) * D, D), D)] = (
                    acc / sums).astype(jnp.bfloat16)
                total = jnp.where(lane == j * group + i, sums, total)
        lse_l[...] = total
        lse_m[...] = top
        return carry

    for j in range(2):
        pass_across(j)

        @pl.when(relays)
        def _(j=j):
            pass_relay(j)

    lax.fori_loop(0, KV, own_step, 0)

    @pl.when(first)
    def _():
        for j in range(AHEAD):
            pass_far(j)
        pass_last(0)

    lax.fori_loop(0, KV, far_step, 0)
    def drain(j, carry):
        own_across(j).wait_send()
        own_partner(j).wait_send()
        across_partner(j).wait_send()
        far_partner(j).wait_send()
        last_partner(j).wait_send()

        @pl.when(ahead)
        def _():
            own_ahead(j).wait_send()

        @pl.when(split)
        def _():
            to_relay(j).wait_send()

        @pl.when(relays)
        def _():
            from_relay(j).wait_send()

        @pl.when(crosses)
        def _():
            own_cross(j).wait_send()

        @pl.when(forwards)
        def _():
            across_ahead(j).wait_send()

        @pl.when(first)
        def _():
            far_across(j).wait_send()

        return carry

    lax.fori_loop(0, KV, drain, 0)


def finish(out_ref, total, top, out_hbm, lse_hbm, lse_s, out_sem, lse_sem):
    width = out_ref.shape[1] // KV
    copies = [
        pltpu.make_async_copy(
            out_ref.at[:, j * width:(j + 1) * width],
            out_hbm.at[:, j * width:(j + 1) * width], out_sem.at[j])
        for j in range(KV)
    ]
    for copy in copies:
        copy.start()
    lse_s[...] = top[...] * (1.0 / math.sqrt(D)) + jnp.log(total[...])
    lse_copy = pltpu.make_async_copy(lse_s, lse_hbm, lse_sem)
    lse_copy.start()
    for copy in copies:
        copy.wait()
    lse_copy.wait()


def body(query, key, value, block_order):
    n_ctx = lax.axis_size("ctx")
    rows = query.shape[0]
    heads = query.shape[1] // D
    group = heads // KV
    keys = SLOTS * rows
    half = group * rows // 2
    vmem, smem, hbm = pltpu.VMEM, pltpu.SMEM, pltpu.HBM
    dma = pltpu.SemaphoreType.DMA
    args = [pltpu.with_memory_space_constraint(x, hbm) for x in (block_order, query, key, value)]
    stats = jax.ShapeDtypeStruct((rows, heads), jnp.float32)
    out, total, top = pl.pallas_call(
        functools.partial(kernel, n_ctx),
        out_shape=(
            jax.ShapeDtypeStruct(query.shape, jnp.bfloat16),
            stats,
            stats,
        ),
        in_specs=[
            pl.BlockSpec(memory_space=hbm),
            pl.BlockSpec(memory_space=hbm),
            pl.BlockSpec(memory_space=hbm),
            pl.BlockSpec(memory_space=hbm),
        ],
        out_specs=(pl.BlockSpec(memory_space=vmem),) * 3,
        scratch_shapes=[
            smem(block_order.shape, jnp.int32),
            vmem((KV, rows, group * D), jnp.bfloat16),
            vmem((KV, 2, keys, D), jnp.bfloat16),
            vmem((KV, 2, rows, D), jnp.bfloat16),
            vmem((2, half, keys // 2), jnp.float32),
            vmem((2, half, keys // 2), jnp.bfloat16),
            vmem((KV, group, rows, D), jnp.float32),
            vmem((KV, 2, half, 2 * D), jnp.float32),
            vmem((2, half, D), jnp.float32),
            vmem((2, half, 2 * D), jnp.float32),
            vmem((keys, D), jnp.bfloat16),
            dma,
            dma((KV,)),
            dma((2, KV)),
            dma((9, KV)),
            dma((9, KV)),
        ],
        compiler_params=pltpu.CompilerParams(
            collective_id=0, has_side_effects=True, vmem_limit_bytes=40 * 1024 * 1024
        ),
        cost_estimate=pl.CostEstimate(
            flops=4 * rows * heads * keys * D,
            bytes_accessed=4 * rows * heads * D,
            transcendentals=rows * heads * keys,
        ),
    )(*args)
    return pl.pallas_call(
        finish,
        out_shape=(jax.ShapeDtypeStruct(query.shape, jnp.bfloat16), stats),
        in_specs=[pl.BlockSpec(memory_space=vmem)] * 3,
        out_specs=(pl.BlockSpec(memory_space=hbm),) * 2,
        scratch_shapes=[vmem((rows, heads), jnp.float32), dma((KV,)), dma],
        compiler_params=pltpu.CompilerParams(vmem_limit_bytes=4 * 1024 * 1024),
    )(out, total, top)


def solution(mesh):
    placed = (P(("head", "ctx"), None), P(("head", "ctx"), None), P(("head", "ctx"), None), P())
    return jax.shard_map(
        body,
        mesh=mesh,
        in_specs=placed,
        out_specs=(P(("head", "ctx"), None), P(("head", "ctx"), None)),
        check_vma=False,
    )
```

```python
import functools
import math

import jax
import jax.numpy as jnp
from jax import lax
from jax.experimental import pallas as pl
from jax.experimental.pallas import tpu as pltpu
from jax.sharding import PartitionSpec as P

D = 128
KV = 8
PLANE = 16
AHEAD = 5
RELAY = 3
DIRECT = 4
READY = 4
SLOTS = 8
HIDDEN = -1e30
MESH = pl.DeviceIdType.MESH


def score(s_s, heads, part, q, picks, k):
    q = jnp.concatenate([q[:, i * D:(i + 1) * D] for i in heads], axis=0)
    s_s[part] = lax.dot_general(
        jnp.concatenate([q, picks], axis=1), k, (((1,), (1,)), ((), ())),
        preferred_element_type=jnp.float32)


def attend_far(base, group, rows, v, m, o, s_s, p_s, f_s, far_s, total, top, out_ref, column=None):
    factor = math.log2(math.e) / math.sqrt(D)
    column = base if column is None else column
    parts = [range(group // 2), range(group // 2, group)]
    lane = lax.broadcasted_iota(jnp.int32, (rows, D), 1)
    for part, heads in enumerate(parts):
        for n, i in enumerate(heads):
            at = slice(n * rows, (n + 1) * rows)
            s = s_s[part, at]
            peak = jnp.maximum(m[i], jnp.max(s, axis=1, keepdims=True))
            p = [jnp.exp2((s[:, at * D:(at + 1) * D] - peak) * factor).astype(jnp.bfloat16)
                 for at in range(s.shape[1] // D)]
            p_s[part, at] = jnp.concatenate(p, axis=1)
            f_s[part, at] = jnp.exp2((m[i] - peak) * factor)
            top = jnp.where(lane == base + i, peak, top)
        far_s[part] = jnp.dot(p_s[part], v, preferred_element_type=jnp.float32)
    for part, heads in enumerate(parts):
        for n, i in enumerate(heads):
            at = slice(n * rows, (n + 1) * rows)
            kept = f_s[part, at]
            acc = o[part, at, :D] * kept + far_s[part, at, :D]
            sums = o[part, at, D:] * kept + far_s[part, at, D:]
            start = (column + i) * D
            if not isinstance(start, int):
                start = pl.multiple_of(start, D)
            out_ref[:, pl.ds(start, D)] = (acc / sums).astype(jnp.bfloat16)
            total = jnp.where(lane == base + i, sums, total)
    return total, top


def kernel(n_ctx, order_hbm, q_hbm, k_hbm, v_hbm, out_ref, lse_l, lse_m,
           q_last, o_last, m_last, kv_last, mask_last,
           order, q_s, kv, relay_s, s_s, p_s, m_s, o_s, f_s, far_s, mask_s,
           order_sem, q_sem, own_sem, send_sem, recv_sem):
    rows = q_hbm.shape[0]
    width = q_hbm.shape[1] // KV
    group = width // D
    hd = lax.axis_index("head")
    ctx = lax.axis_index("ctx")
    z, c = hd // 2, hd % 2
    nxt, prv = (ctx + 1) % n_ctx, (ctx + n_ctx - 1) % n_ctx
    partner = (2 * z + 1 - c, ctx)
    across = (2 * (1 - z) + c, ctx)
    diagonal = (2 * (1 - z) + 1 - c, ctx)
    first = ctx % PLANE == 0
    last = ctx % PLANE == PLANE - 1
    shard = ctx % PLANE
    spare = shard == RELAY
    relays = jnp.logical_and(spare, z == 1)
    split = jnp.logical_and(last, z == 1)
    ahead = jnp.logical_not(split)
    crowded = jnp.logical_and(last, z == 0)
    by_relay = jnp.logical_and(first, z == 1)
    forwards = jnp.logical_or(first, spare)
    crosses = jnp.logical_not(jnp.logical_or(forwards, last))
    before = prv % PLANE
    from_cross = jnp.logical_not(jnp.logical_or(
        jnp.logical_or(before == 0, before == PLANE - 1), before == RELAY))
    own_target = (hd, nxt)
    cross_target = (2 * (1 - z) + c, nxt)
    cross_source = (2 * (1 - z) + c, prv)
    source = (hd, jnp.where(by_relay, prv - (PLANE - 1 - RELAY), prv))
    relay_source = (hd, ctx - shard + PLANE - 1)
    relay_target = (hd, (ctx - shard + PLANE) % n_ctx)

    def chunk(slot, j):
        return kv.at[j, :, pl.ds(slot * rows, rows)]

    def message(kind, j, src, dst, device):
        return pltpu.make_async_remote_copy(
            src_ref=chunk(src, j), dst_ref=chunk(dst, j),
            send_sem=send_sem.at[kind, j], recv_sem=recv_sem.at[dst, j],
            device_id=device, device_id_type=MESH)

    def own_partner(j):
        return message(1, j, 0, 1, partner)

    def own_across(j):
        return message(2, j, 0, 2, across)

    def across_partner(j):
        return message(3, j, 2, 3, partner)

    def own_ahead(j):
        return message(4, j, 0, 4, own_target)

    def far_partner(j):
        return message(5, j, 4, 5, partner)

    def across_ahead(j):
        return message(6, j, 2, 6, own_target)

    def to_relay(j):
        stop = ctx - (PLANE - 1 - RELAY)
        return pltpu.make_async_remote_copy(
            src_ref=chunk(0, j), dst_ref=relay_s.at[j],
            send_sem=send_sem.at[4, j], recv_sem=recv_sem.at[8, j],
            device_id=(hd, stop), device_id_type=MESH)

    def from_relay(j):
        return pltpu.make_async_remote_copy(
            src_ref=relay_s.at[j], dst_ref=chunk(4, j),
            send_sem=send_sem.at[8, j], recv_sem=recv_sem.at[4, j],
            device_id=relay_target, device_id_type=MESH)

    def own_cross(j):
        return message(6, j, 0, 6, cross_target)

    def far_across(j):
        return message(0, j, 4, 6, across)

    def last_partner(j):
        return message(7, j, 6, 7, partner)

    def far_diagonal(j):
        return message(7, j, 4, 7, diagonal)

    def direct(j):
        return jnp.logical_and(first, j >= DIRECT)

    def arrived(slot, j):
        message(1, j, 0, slot, partner).wait_recv()

    def q_copy(j):
        return pltpu.make_async_copy(
            q_hbm.at[:, pl.ds(pl.multiple_of(j * width, width), width)], q_s.at[j], q_sem.at[j])

    def own_copy(i, j):
        ref = (k_hbm, v_hbm)[i]
        return pltpu.make_async_copy(
            ref.at[:, pl.ds(pl.multiple_of(j * D, D), D)],
            kv.at[j, i, pl.ds(0, rows)], own_sem.at[i, j])

    for j in range(KV):
        own_copy(0, j).start()
        own_copy(1, j).start()
    order_copy = pltpu.make_async_copy(order_hbm, order, order_sem)
    order_copy.start()
    for j in range(KV):
        q_copy(j).start()

    barrier = pltpu.get_barrier_semaphore()

    def greet(device):
        pl.semaphore_signal(barrier, inc=1, device_id=device, device_id_type=MESH)

    greet(partner)
    greet(across)
    greet(source)

    @pl.when(relays)
    def _():
        greet(relay_source)

    @pl.when(first)
    def _():
        greet(diagonal)

    @pl.when(from_cross)
    def _():
        greet(cross_source)

    def one(flag):
        return jnp.where(flag, 1, 0)

    pl.semaphore_wait(
        barrier, 2 + one(ahead) + one(split) + one(crosses) + one(relays) + one(first))

    for j in range(KV):
        own_copy(0, j).wait()
        own_copy(1, j).wait()

        @pl.when(jnp.logical_not(crowded))
        def _(j=j):
            own_across(j).start()

        @pl.when(crosses)
        def _(j=j):
            own_cross(j).start()

        @pl.when(ahead)
        def _(j=j):
            own_ahead(j).start()

        @pl.when(split)
        def _(j=j):
            to_relay(j).start()

        own_partner(j).start()

    @pl.when(crowded)
    def _():
        for j in range(KV):
            own_across(j).start()

    order_copy.wait()
    query_pos = order[hd * n_ctx + ctx] * rows + lax.broadcasted_iota(jnp.int32, (rows, D), 1)
    for slot in range(SLOTS):
        holder = 2 * (z if slot % 4 < 2 else 1 - z) + (c if slot % 2 == 0 else 1 - c)
        block = order[holder * n_ctx + (ctx if slot < 4 else prv)]
        key_pos = block * rows + lax.broadcasted_iota(jnp.int32, (rows, D), 0)
        mask_s[slot * rows:(slot + 1) * rows, :] = jnp.where(
            key_pos <= query_pos, 0.0, HIDDEN).astype(jnp.bfloat16)
    lane = lax.broadcasted_iota(jnp.int32, (rows, D), 1)
    row = lax.broadcasted_iota(jnp.int32, (rows, D), 0)
    pick = jnp.where(lane == row, 1.0, 0.0).astype(jnp.bfloat16)
    lse_l[...] = jnp.ones_like(lse_l)
    lse_m[...] = jnp.zeros_like(lse_m)

    def pass_across(j):
        arrived(2, j)

        @pl.when(forwards)
        def _():
            across_ahead(j).start()

        across_partner(j).start()

    def pass_far(j):
        arrived(4, j)

        @pl.when(first)
        def _():
            far_across(j).start()

        @pl.when(direct(j))
        def _():
            far_diagonal(j).start()

        far_partner(j).start()

    def pass_relay(j):
        to_relay(j).wait_recv()
        from_relay(j).start()

    def pass_last(j):
        @pl.when(jnp.logical_not(direct(j)))
        def _():
            arrived(6, j)
            last_partner(j).start()

    scale = 1.0 / math.sqrt(D)
    floor = -10000.0 / scale
    factor = scale * math.log2(math.e)
    keys = SLOTS // 2 * rows
    parts = [range(group // 2), range(group // 2, group)]
    picks = jnp.concatenate([pick] * (group // 2), axis=0)
    ones = jnp.ones((keys, D), jnp.bfloat16)

    def scores(j, shard):
        seen = pl.ds(shard * keys, keys)
        k = jnp.concatenate([kv[j, 0, seen], mask_s[seen]], axis=1)
        for part, heads in enumerate(parts):
            score(s_s, heads, part, q_s.at[j], picks, k)

    def value(j, shard):
        return jnp.concatenate([kv[j, 1, shard * keys:(shard + 1) * keys], ones], axis=1)

    def own_step(j, carry):
        @pl.when(j < KV - 2)
        def _():
            pass_across(j + 2)

            @pl.when(relays)
            def _():
                pass_relay(j + 2)

        @pl.when(jnp.logical_and(jnp.logical_not(first), j >= KV - READY))
        def _():
            pass_far(j - (KV - READY))
            pass_last(j - (KV - READY))

        q_copy(j).wait()
        arrived(1, j)
        arrived(3, j)
        scores(j, 0)
        v = value(j, 0)
        for part, heads in enumerate(parts):
            for n, i in enumerate(heads):
                at = slice(n * rows, (n + 1) * rows)
                s = s_s[part, at]
                peak = jnp.maximum(jnp.max(s, axis=1, keepdims=True), floor)
                p_s[part, at] = jnp.exp2((s - peak) * factor).astype(jnp.bfloat16)
                m_s[j, i] = jnp.broadcast_to(peak, (rows, D))
            o_s[j, part] = jnp.dot(p_s[part], v, preferred_element_type=jnp.float32)
        return carry

    def far_step(j, carry):
        later = jnp.logical_not(first)

        @pl.when(jnp.logical_and(first, j < KV - AHEAD))
        def _():
            pass_far(j + AHEAD)

        @pl.when(jnp.logical_and(later, jnp.logical_and(j >= READY - 1, j < KV - 1)))
        def _():
            pass_far(j + 1)

        @pl.when(jnp.logical_and(jnp.logical_or(first, j >= READY - 1), j < KV - 1))
        def _():
            pass_last(j + 1)

        @pl.when(direct(j))
        def _():
            arrived(6, j)

        arrived(5, j)
        arrived(7, j)
        scores(j, 1)
        total, top = attend_far(
            j * group, group, rows, value(j, 1), m_s.at[j], o_s.at[j], s_s, p_s, f_s, far_s,
            lse_l[...], lse_m[...], out_ref)
        lse_l[...] = total
        lse_m[...] = top
        return carry

    for j in range(2):
        pass_across(j)

        @pl.when(relays)
        def _(j=j):
            pass_relay(j)

    lax.fori_loop(0, KV, own_step, 0)

    q_last[...] = q_s[KV - 1]
    o_last[...] = o_s[KV - 1]
    m_last[...] = m_s[KV - 1]
    mask_last[...] = mask_s[keys:]

    @pl.when(first)
    def _():
        for j in range(AHEAD):
            pass_far(j)
        pass_last(0)

    lax.fori_loop(0, KV - 1, far_step, 0)

    end = KV - 1

    @pl.when(direct(end))
    def _():
        arrived(6, end)

    arrived(5, end)
    arrived(7, end)
    kv_last[...] = kv[end, :, keys:]
    def drain(j, carry):
        own_across(j).wait_send()
        own_partner(j).wait_send()
        across_partner(j).wait_send()
        far_partner(j).wait_send()
        last_partner(j).wait_send()

        @pl.when(ahead)
        def _():
            own_ahead(j).wait_send()

        @pl.when(split)
        def _():
            to_relay(j).wait_send()

        @pl.when(relays)
        def _():
            from_relay(j).wait_send()

        @pl.when(crosses)
        def _():
            own_cross(j).wait_send()

        @pl.when(forwards)
        def _():
            across_ahead(j).wait_send()

        @pl.when(first)
        def _():
            far_across(j).wait_send()

        return carry

    lax.fori_loop(0, KV, drain, 0)


def finish(out_ref, total, top, q, o, m, kv, mask, out_hbm, lse_hbm,
           tail_s, lse_s, s_s, p_s, f_s, far_s, out_sem, tail_sem, lse_sem):
    rows, width = q.shape
    group = width // D
    done = out_ref.shape[1] // width
    copies = [
        pltpu.make_async_copy(
            out_ref.at[:, j * width:(j + 1) * width],
            out_hbm.at[:, j * width:(j + 1) * width], out_sem.at[j])
        for j in range(done)
    ]
    for copy in copies:
        copy.start()
    lane = lax.broadcasted_iota(jnp.int32, (rows, D), 1)
    row = lax.broadcasted_iota(jnp.int32, (rows, D), 0)
    picks = jnp.concatenate(
        [jnp.where(lane == row, 1.0, 0.0).astype(jnp.bfloat16)] * (group // 2), axis=0)
    k = jnp.concatenate([kv[0], mask[...]], axis=1)
    v = jnp.concatenate([kv[1], jnp.ones(mask.shape, jnp.bfloat16)], axis=1)
    for part in range(2):
        score(s_s, range(part * group // 2, (part + 1) * group // 2), part, q, picks, k)
    sums, peaks = attend_far(
        done * group, group, rows, v, m, o, s_s, p_s, f_s, far_s,
        total[...], top[...], tail_s, column=0)
    tail = pltpu.make_async_copy(
        tail_s, out_hbm.at[:, done * width:(done + 1) * width], tail_sem)
    tail.start()
    lse_s[...] = peaks * (1.0 / math.sqrt(D)) + jnp.log(sums)
    lse_copy = pltpu.make_async_copy(lse_s, lse_hbm, lse_sem)
    lse_copy.start()
    for copy in copies:
        copy.wait()
    tail.wait()
    lse_copy.wait()


def body(query, key, value, block_order):
    n_ctx = lax.axis_size("ctx")
    rows = query.shape[0]
    heads = query.shape[1] // D
    group = heads // KV
    keys = SLOTS * rows
    half = group * rows // 2
    vmem, smem, hbm = pltpu.VMEM, pltpu.SMEM, pltpu.HBM
    dma = pltpu.SemaphoreType.DMA
    args = [pltpu.with_memory_space_constraint(x, hbm) for x in (block_order, query, key, value)]
    stats = jax.ShapeDtypeStruct((rows, heads), jnp.float32)
    work = [
        vmem((2, half, keys // 2), jnp.float32),
        vmem((2, half, keys // 2), jnp.bfloat16),
        vmem((2, half, D), jnp.float32),
        vmem((2, half, 2 * D), jnp.float32),
    ]
    handed = pl.pallas_call(
        functools.partial(kernel, n_ctx),
        out_shape=(
            jax.ShapeDtypeStruct((rows, (KV - 1) * group * D), jnp.bfloat16),
            stats,
            stats,
            jax.ShapeDtypeStruct((rows, group * D), jnp.bfloat16),
            jax.ShapeDtypeStruct((2, half, 2 * D), jnp.float32),
            jax.ShapeDtypeStruct((group, rows, D), jnp.float32),
            jax.ShapeDtypeStruct((2, keys // 2, D), jnp.bfloat16),
            jax.ShapeDtypeStruct((keys // 2, D), jnp.bfloat16),
        ),
        in_specs=[
            pl.BlockSpec(memory_space=hbm),
            pl.BlockSpec(memory_space=hbm),
            pl.BlockSpec(memory_space=hbm),
            pl.BlockSpec(memory_space=hbm),
        ],
        out_specs=(pl.BlockSpec(memory_space=vmem),) * 8,
        scratch_shapes=[
            smem(block_order.shape, jnp.int32),
            vmem((KV, rows, group * D), jnp.bfloat16),
            vmem((KV, 2, keys, D), jnp.bfloat16),
            vmem((KV, 2, rows, D), jnp.bfloat16),
            vmem((2, half, keys // 2), jnp.float32),
            vmem((2, half, keys // 2), jnp.bfloat16),
            vmem((KV, group, rows, D), jnp.float32),
            vmem((KV, 2, half, 2 * D), jnp.float32),
            vmem((2, half, D), jnp.float32),
            vmem((2, half, 2 * D), jnp.float32),
            vmem((keys, D), jnp.bfloat16),
            dma,
            dma((KV,)),
            dma((2, KV)),
            dma((9, KV)),
            dma((9, KV)),
        ],
        compiler_params=pltpu.CompilerParams(
            collective_id=0, has_side_effects=True, vmem_limit_bytes=40 * 1024 * 1024
        ),
        cost_estimate=pl.CostEstimate(
            flops=4 * rows * heads * keys * D,
            bytes_accessed=4 * rows * heads * D,
            transcendentals=rows * heads * keys,
        ),
    )(*args)
    return pl.pallas_call(
        finish,
        out_shape=(jax.ShapeDtypeStruct(query.shape, jnp.bfloat16), stats),
        in_specs=[pl.BlockSpec(memory_space=vmem)] * 8,
        out_specs=(pl.BlockSpec(memory_space=hbm),) * 2,
        scratch_shapes=[
            vmem((rows, group * D), jnp.bfloat16),
            vmem((rows, heads), jnp.float32),
            *work,
            dma((KV - 1,)),
            dma,
            dma,
        ],
        compiler_params=pltpu.CompilerParams(vmem_limit_bytes=12 * 1024 * 1024),
    )(*handed)


def solution(mesh):
    placed = (P(("head", "ctx"), None), P(("head", "ctx"), None), P(("head", "ctx"), None), P())
    return jax.shard_map(
        body,
        mesh=mesh,
        in_specs=placed,
        out_specs=(P(("head", "ctx"), None), P(("head", "ctx"), None)),
        check_vma=False,
    )
```

```python
import functools
import math

import jax
import jax.numpy as jnp
from jax import lax
from jax.experimental import pallas as pl
from jax.experimental.pallas import tpu as pltpu
from jax.sharding import PartitionSpec as P

D = 128
KV = 8
PLANE = 16
AHEAD = 6
RELAY = 3
DIRECT = 4
READY = 4
SLOTS = 8
HIDDEN = -1e30
MESH = pl.DeviceIdType.MESH


def score(s_s, heads, part, q, picks, k):
    q = jnp.concatenate([q[:, i * D:(i + 1) * D] for i in heads], axis=0)
    s_s[part] = lax.dot_general(
        jnp.concatenate([q, picks], axis=1), k, (((1,), (1,)), ((), ())),
        preferred_element_type=jnp.float32)


def attend_far(base, group, rows, v, m, o, s_s, p_s, f_s, far_s, total, top, out_ref, column=None):
    factor = math.log2(math.e) / math.sqrt(D)
    column = base if column is None else column
    parts = [range(group // 2), range(group // 2, group)]
    lane = lax.broadcasted_iota(jnp.int32, (rows, D), 1)
    for part, heads in enumerate(parts):
        for n, i in enumerate(heads):
            at = slice(n * rows, (n + 1) * rows)
            s = s_s[part, at]
            peak = jnp.maximum(m[i], jnp.max(s, axis=1, keepdims=True))
            p = [jnp.exp2((s[:, at * D:(at + 1) * D] - peak) * factor).astype(jnp.bfloat16)
                 for at in range(s.shape[1] // D)]
            p_s[part, at] = jnp.concatenate(p, axis=1)
            f_s[part, at] = jnp.exp2((m[i] - peak) * factor)
            top = jnp.where(lane == base + i, peak, top)
        far_s[part] = jnp.dot(p_s[part], v, preferred_element_type=jnp.float32)
    for part, heads in enumerate(parts):
        for n, i in enumerate(heads):
            at = slice(n * rows, (n + 1) * rows)
            kept = f_s[part, at]
            acc = o[part, at, :D] * kept + far_s[part, at, :D]
            sums = o[part, at, D:] * kept + far_s[part, at, D:]
            start = (column + i) * D
            if not isinstance(start, int):
                start = pl.multiple_of(start, D)
            out_ref[:, pl.ds(start, D)] = (acc / sums).astype(jnp.bfloat16)
            total = jnp.where(lane == base + i, sums, total)
    return total, top


def kernel(n_ctx, order_hbm, q_hbm, k_hbm, v_hbm, out_ref, lse_l, lse_m,
           q_last, o_last, m_last, kv_last, mask_last,
           order, q_s, kv, relay_s, s_s, p_s, m_s, o_s, f_s, far_s, mask_s,
           order_sem, q_sem, own_sem, send_sem, recv_sem):
    rows = q_hbm.shape[0]
    width = q_hbm.shape[1] // KV
    group = width // D
    hd = lax.axis_index("head")
    ctx = lax.axis_index("ctx")
    z, c = hd // 2, hd % 2
    nxt, prv = (ctx + 1) % n_ctx, (ctx + n_ctx - 1) % n_ctx
    partner = (2 * z + 1 - c, ctx)
    across = (2 * (1 - z) + c, ctx)
    diagonal = (2 * (1 - z) + 1 - c, ctx)
    first = ctx % PLANE == 0
    last = ctx % PLANE == PLANE - 1
    shard = ctx % PLANE
    spare = shard == RELAY
    relays = jnp.logical_and(spare, z == 1)
    split = jnp.logical_and(last, z == 1)
    ahead = jnp.logical_not(split)
    crowded = jnp.logical_and(last, z == 0)
    by_relay = jnp.logical_and(first, z == 1)
    forwards = jnp.logical_or(first, spare)
    crosses = jnp.logical_not(jnp.logical_or(forwards, last))
    before = prv % PLANE
    from_cross = jnp.logical_not(jnp.logical_or(
        jnp.logical_or(before == 0, before == PLANE - 1), before == RELAY))
    own_target = (hd, nxt)
    cross_target = (2 * (1 - z) + c, nxt)
    cross_source = (2 * (1 - z) + c, prv)
    source = (hd, jnp.where(by_relay, prv - (PLANE - 1 - RELAY), prv))
    relay_source = (hd, ctx - shard + PLANE - 1)
    relay_target = (hd, (ctx - shard + PLANE) % n_ctx)

    def chunk(slot, j):
        return kv.at[j, :, pl.ds(slot * rows, rows)]

    def message(kind, j, src, dst, device):
        return pltpu.make_async_remote_copy(
            src_ref=chunk(src, j), dst_ref=chunk(dst, j),
            send_sem=send_sem.at[kind, j], recv_sem=recv_sem.at[dst, j],
            device_id=device, device_id_type=MESH)

    def own_partner(j):
        return message(1, j, 0, 1, partner)

    def own_across(j):
        return message(2, j, 0, 2, across)

    def across_partner(j):
        return message(3, j, 2, 3, partner)

    def own_ahead(j):
        return message(4, j, 0, 4, own_target)

    def far_partner(j):
        return message(5, j, 4, 5, partner)

    def across_ahead(j):
        return message(6, j, 2, 6, own_target)

    def to_relay(j):
        stop = (ctx + n_ctx - (PLANE - 1 - RELAY)) % n_ctx
        return pltpu.make_async_remote_copy(
            src_ref=chunk(0, j), dst_ref=relay_s.at[j],
            send_sem=send_sem.at[4, j], recv_sem=recv_sem.at[8, j],
            device_id=(hd, stop), device_id_type=MESH)

    def from_relay(j):
        return pltpu.make_async_remote_copy(
            src_ref=relay_s.at[j], dst_ref=chunk(4, j),
            send_sem=send_sem.at[8, j], recv_sem=recv_sem.at[4, j],
            device_id=relay_target, device_id_type=MESH)

    def own_cross(j):
        return message(6, j, 0, 6, cross_target)

    def far_across(j):
        return message(0, j, 4, 6, across)

    def last_partner(j):
        return message(7, j, 6, 7, partner)

    def far_diagonal(j):
        return message(7, j, 4, 7, diagonal)

    def direct(j):
        return jnp.logical_and(first, j >= DIRECT)

    def arrived(slot, j):
        message(1, j, 0, slot, partner).wait_recv()

    def q_copy(j):
        return pltpu.make_async_copy(
            q_hbm.at[:, pl.ds(pl.multiple_of(j * width, width), width)], q_s.at[j], q_sem.at[j])

    def own_copy(i, j):
        ref = (k_hbm, v_hbm)[i]
        return pltpu.make_async_copy(
            ref.at[:, pl.ds(pl.multiple_of(j * D, D), D)],
            kv.at[j, i, pl.ds(0, rows)], own_sem.at[i, j])

    for j in range(KV):
        own_copy(0, j).start()
        own_copy(1, j).start()
    order_copy = pltpu.make_async_copy(order_hbm, order, order_sem)
    order_copy.start()
    for j in range(KV):
        q_copy(j).start()

    barrier = pltpu.get_barrier_semaphore()

    def greet(device):
        pl.semaphore_signal(barrier, inc=1, device_id=device, device_id_type=MESH)

    greet(partner)
    greet(across)
    greet(source)

    @pl.when(relays)
    def _():
        greet(relay_source)

    @pl.when(first)
    def _():
        greet(diagonal)

    @pl.when(from_cross)
    def _():
        greet(cross_source)

    def one(flag):
        return jnp.where(flag, 1, 0)

    pl.semaphore_wait(
        barrier, 2 + one(ahead) + one(split) + one(crosses) + one(relays) + one(first))

    for j in range(KV):
        own_copy(0, j).wait()
        own_copy(1, j).wait()

        @pl.when(jnp.logical_not(crowded))
        def _(j=j):
            own_across(j).start()

        @pl.when(crosses)
        def _(j=j):
            own_cross(j).start()

        @pl.when(ahead)
        def _(j=j):
            own_ahead(j).start()

        @pl.when(split)
        def _(j=j):
            to_relay(j).start()

        own_partner(j).start()

    @pl.when(crowded)
    def _():
        for j in range(KV):
            own_across(j).start()

    order_copy.wait()
    query_pos = order[hd * n_ctx + ctx] * rows + lax.broadcasted_iota(jnp.int32, (rows, D), 1)
    for slot in range(SLOTS):
        holder = 2 * (z if slot % 4 < 2 else 1 - z) + (c if slot % 2 == 0 else 1 - c)
        block = order[holder * n_ctx + (ctx if slot < 4 else prv)]
        key_pos = block * rows + lax.broadcasted_iota(jnp.int32, (rows, D), 0)
        mask_s[slot * rows:(slot + 1) * rows, :] = jnp.where(
            key_pos <= query_pos, 0.0, HIDDEN).astype(jnp.bfloat16)
    lane = lax.broadcasted_iota(jnp.int32, (rows, D), 1)
    row = lax.broadcasted_iota(jnp.int32, (rows, D), 0)
    pick = jnp.where(lane == row, 1.0, 0.0).astype(jnp.bfloat16)
    lse_l[...] = jnp.ones_like(lse_l)
    lse_m[...] = jnp.zeros_like(lse_m)

    def pass_across(j):
        arrived(2, j)

        @pl.when(forwards)
        def _():
            across_ahead(j).start()

        across_partner(j).start()

    def pass_far(j):
        arrived(4, j)

        @pl.when(first)
        def _():
            far_across(j).start()

        @pl.when(direct(j))
        def _():
            far_diagonal(j).start()

        far_partner(j).start()

    def pass_relay(j):
        to_relay(j).wait_recv()
        from_relay(j).start()

    def pass_last(j):
        @pl.when(jnp.logical_not(direct(j)))
        def _():
            arrived(6, j)
            last_partner(j).start()

    scale = 1.0 / math.sqrt(D)
    floor = -10000.0 / scale
    factor = scale * math.log2(math.e)
    keys = SLOTS // 2 * rows
    parts = [range(group // 2), range(group // 2, group)]
    picks = jnp.concatenate([pick] * (group // 2), axis=0)
    ones = jnp.ones((keys, D), jnp.bfloat16)

    def scores(j, shard):
        seen = pl.ds(shard * keys, keys)
        k = jnp.concatenate([kv[j, 0, seen], mask_s[seen]], axis=1)
        for part, heads in enumerate(parts):
            score(s_s, heads, part, q_s.at[j], picks, k)

    def value(j, shard):
        return jnp.concatenate([kv[j, 1, shard * keys:(shard + 1) * keys], ones], axis=1)

    def own_step(j, carry):
        @pl.when(j < KV - 2)
        def _():
            pass_across(j + 2)

            @pl.when(relays)
            def _():
                pass_relay(j + 2)

        @pl.when(jnp.logical_and(jnp.logical_not(first), j >= KV - READY))
        def _():
            pass_far(j - (KV - READY))
            pass_last(j - (KV - READY))

        q_copy(j).wait()
        arrived(1, j)
        arrived(3, j)
        scores(j, 0)
        v = value(j, 0)
        for part, heads in enumerate(parts):
            for n, i in enumerate(heads):
                at = slice(n * rows, (n + 1) * rows)
                s = s_s[part, at]
                peak = jnp.maximum(jnp.max(s, axis=1, keepdims=True), floor)
                p_s[part, at] = jnp.exp2((s - peak) * factor).astype(jnp.bfloat16)
                m_s[j, i] = jnp.broadcast_to(peak, (rows, D))
            o_s[j, part] = jnp.dot(p_s[part], v, preferred_element_type=jnp.float32)
        return carry

    def far_step(j, carry):
        later = jnp.logical_not(first)

        @pl.when(jnp.logical_and(first, j < KV - AHEAD))
        def _():
            pass_far(j + AHEAD)

        @pl.when(jnp.logical_and(later, jnp.logical_and(j >= READY - 1, j < KV - 1)))
        def _():
            pass_far(j + 1)

        @pl.when(jnp.logical_and(jnp.logical_or(first, j >= READY - 1), j < KV - 1))
        def _():
            pass_last(j + 1)

        @pl.when(direct(j))
        def _():
            arrived(6, j)

        arrived(5, j)
        arrived(7, j)
        scores(j, 1)
        total, top = attend_far(
            j * group, group, rows, value(j, 1), m_s.at[j], o_s.at[j], s_s, p_s, f_s, far_s,
            lse_l[...], lse_m[...], out_ref)
        lse_l[...] = total
        lse_m[...] = top
        return carry

    for j in range(2):
        pass_across(j)

        @pl.when(relays)
        def _(j=j):
            pass_relay(j)

    lax.fori_loop(0, KV, own_step, 0)

    q_last[...] = q_s[KV - 1]
    o_last[...] = o_s[KV - 1]
    m_last[...] = m_s[KV - 1]
    mask_last[...] = mask_s[keys:]

    @pl.when(first)
    def _():
        for j in range(AHEAD):
            pass_far(j)
        pass_last(0)

    lax.fori_loop(0, KV - 1, far_step, 0)

    def drain(j, carry):
        own_across(j).wait_send()
        own_partner(j).wait_send()
        across_partner(j).wait_send()
        far_partner(j).wait_send()
        last_partner(j).wait_send()

        @pl.when(ahead)
        def _():
            own_ahead(j).wait_send()

        @pl.when(split)
        def _():
            to_relay(j).wait_send()

        @pl.when(relays)
        def _():
            from_relay(j).wait_send()

        @pl.when(crosses)
        def _():
            own_cross(j).wait_send()

        @pl.when(forwards)
        def _():
            across_ahead(j).wait_send()

        @pl.when(first)
        def _():
            far_across(j).wait_send()

        return carry

    lax.fori_loop(0, KV - 1, drain, 0)

    end = KV - 1

    @pl.when(direct(end))
    def _():
        arrived(6, end)

    arrived(5, end)
    arrived(7, end)
    kv_last[...] = kv[end, :, keys:]
    drain(end, 0)


def finish(out_ref, total, top, q, o, m, kv, mask, out_hbm, lse_hbm,
           tail_s, lse_s, s_s, p_s, f_s, far_s, out_sem, tail_sem, lse_sem):
    rows, width = q.shape
    group = width // D
    done = out_ref.shape[1] // width
    copies = [
        pltpu.make_async_copy(
            out_ref.at[:, j * width:(j + 1) * width],
            out_hbm.at[:, j * width:(j + 1) * width], out_sem.at[j])
        for j in range(done)
    ]
    for copy in copies:
        copy.start()
    lane = lax.broadcasted_iota(jnp.int32, (rows, D), 1)
    row = lax.broadcasted_iota(jnp.int32, (rows, D), 0)
    picks = jnp.concatenate(
        [jnp.where(lane == row, 1.0, 0.0).astype(jnp.bfloat16)] * (group // 2), axis=0)
    k = jnp.concatenate([kv[0], mask[...]], axis=1)
    v = jnp.concatenate([kv[1], jnp.ones(mask.shape, jnp.bfloat16)], axis=1)
    for part in range(2):
        score(s_s, range(part * group // 2, (part + 1) * group // 2), part, q, picks, k)
    sums, peaks = attend_far(
        done * group, group, rows, v, m, o, s_s, p_s, f_s, far_s,
        total[...], top[...], tail_s, column=0)
    tail = pltpu.make_async_copy(
        tail_s, out_hbm.at[:, done * width:(done + 1) * width], tail_sem)
    tail.start()
    lse_s[...] = peaks * (1.0 / math.sqrt(D)) + jnp.log(sums)
    lse_copy = pltpu.make_async_copy(lse_s, lse_hbm, lse_sem)
    lse_copy.start()
    for copy in copies:
        copy.wait()
    tail.wait()
    lse_copy.wait()


def body(query, key, value, block_order):
    n_ctx = lax.axis_size("ctx")
    rows = query.shape[0]
    heads = query.shape[1] // D
    group = heads // KV
    keys = SLOTS * rows
    half = group * rows // 2
    vmem, smem, hbm = pltpu.VMEM, pltpu.SMEM, pltpu.HBM
    dma = pltpu.SemaphoreType.DMA
    args = [pltpu.with_memory_space_constraint(x, hbm) for x in (block_order, query, key, value)]
    stats = jax.ShapeDtypeStruct((rows, heads), jnp.float32)
    work = [
        vmem((2, half, keys // 2), jnp.float32),
        vmem((2, half, keys // 2), jnp.bfloat16),
        vmem((2, half, D), jnp.float32),
        vmem((2, half, 2 * D), jnp.float32),
    ]
    handed = pl.pallas_call(
        functools.partial(kernel, n_ctx),
        out_shape=(
            jax.ShapeDtypeStruct((rows, (KV - 1) * group * D), jnp.bfloat16),
            stats,
            stats,
            jax.ShapeDtypeStruct((rows, group * D), jnp.bfloat16),
            jax.ShapeDtypeStruct((2, half, 2 * D), jnp.float32),
            jax.ShapeDtypeStruct((group, rows, D), jnp.float32),
            jax.ShapeDtypeStruct((2, keys // 2, D), jnp.bfloat16),
            jax.ShapeDtypeStruct((keys // 2, D), jnp.bfloat16),
        ),
        in_specs=[
            pl.BlockSpec(memory_space=hbm),
            pl.BlockSpec(memory_space=hbm),
            pl.BlockSpec(memory_space=hbm),
            pl.BlockSpec(memory_space=hbm),
        ],
        out_specs=(pl.BlockSpec(memory_space=vmem),) * 8,
        scratch_shapes=[
            smem(block_order.shape, jnp.int32),
            vmem((KV, rows, group * D), jnp.bfloat16),
            vmem((KV, 2, keys, D), jnp.bfloat16),
            vmem((KV, 2, rows, D), jnp.bfloat16),
            vmem((2, half, keys // 2), jnp.float32),
            vmem((2, half, keys // 2), jnp.bfloat16),
            vmem((KV, group, rows, D), jnp.float32),
            vmem((KV, 2, half, 2 * D), jnp.float32),
            vmem((2, half, D), jnp.float32),
            vmem((2, half, 2 * D), jnp.float32),
            vmem((keys, D), jnp.bfloat16),
            dma,
            dma((KV,)),
            dma((2, KV)),
            dma((9, KV)),
            dma((9, KV)),
        ],
        compiler_params=pltpu.CompilerParams(
            collective_id=0, has_side_effects=True, vmem_limit_bytes=40 * 1024 * 1024
        ),
        cost_estimate=pl.CostEstimate(
            flops=4 * rows * heads * keys * D,
            bytes_accessed=4 * rows * heads * D,
            transcendentals=rows * heads * keys,
        ),
    )(*args)
    return pl.pallas_call(
        finish,
        out_shape=(jax.ShapeDtypeStruct(query.shape, jnp.bfloat16), stats),
        in_specs=[pl.BlockSpec(memory_space=vmem)] * 8,
        out_specs=(pl.BlockSpec(memory_space=hbm),) * 2,
        scratch_shapes=[
            vmem((rows, group * D), jnp.bfloat16),
            vmem((rows, heads), jnp.float32),
            *work,
            dma((KV - 1,)),
            dma,
            dma,
        ],
        compiler_params=pltpu.CompilerParams(vmem_limit_bytes=12 * 1024 * 1024),
    )(*handed)


def solution(mesh):
    placed = (P(("head", "ctx"), None), P(("head", "ctx"), None), P(("head", "ctx"), None), P())
    return jax.shard_map(
        body,
        mesh=mesh,
        in_specs=placed,
        out_specs=(P(("head", "ctx"), None), P(("head", "ctx"), None)),
        check_vma=False,
    )
```
